128 devices in a mesh: seq: 32 (over y, z_lo, x), tp: 4 (over z_hi, core).
Axes of the slice: x: 4, y: 4, z: 4 (z_hi: 2, z_lo: 2; z = z_hi * 2 + z_lo), core: 2. Of those that a mesh axis runs over, the one named last changes fastest.
Arguments:
- tokens: bfloat16 [16384, 3584], P('seq'), may hold values from -6 to 6
- norm_gain: float32 [3584], replicated, may hold values from 0.5 to 1.5
- q_weight: bfloat16 [3584, 3584], P(None, 'tp'), may hold values from -0.09375 to 0.09375
- q_bias: float32 [3584], P('tp'), may hold values from -9 to 9
- k_weight: bfloat16 [3584, 512], P(None, 'tp'), may hold values from -0.09375 to 0.09375
- k_bias: float32 [512], P('tp'), may hold values from -9 to 9
- v_weight: bfloat16 [3584, 512], P(None, 'tp'), may hold values from -0.09375 to 0.09375
- v_bias: float32 [512], P('tp'), may hold values from -5 to 5
- o_weight: bfloat16 [3584, 3584], P('tp'), may hold values from -0.09375 to 0.09375
- doc_ids: int32 [16384], replicated, may hold values from 0 to 7, never falling along the last dimension, each value on 1 to 8704 neighbouring positions
Outputs:
- attn_out: bfloat16 [16384, 3584], P('seq', 'tp')
The draws below stay inside these ranges and needn't reach their ends.
Inputs may be any that keep to these rules, and one draw needn't show every extreme that they name: `doc_ids`: document numbers never fall along the sequence; each document holds 1 to 8704 tokens and one holds exactly that many.
All inputs are finite; a program needn't handle non-finite values.
Results may differ from the reference program's by a relative error of at most 0.012.
Values may be sent and summed in bfloat16 or wider, within the bound.
A program may use at most 128 MiB of HBM per device.

```python
import math
import jax
import jax.numpy as jnp
import numpy as np
from jax import lax

D = 3584
HQ = 28
KVH = 4
HD = 128
TOK_DEV = 512
DOCS = 8
TOKENS = 16384
N_TP = 4


def bias_noise(key, count):
    return jnp.clip(jax.random.normal(key, (count,), jnp.float32), -5.0, 5.0)


def bias_plan(key):
    base = jax.random.fold_in(key, 9157)
    signs = (jax.random.randint(jax.random.fold_in(base, 1), (HD,), 0, 2) * 2 - 1).astype(jnp.float32)
    across = jnp.arange(HD) % (HD // 2)
    pattern = jnp.where(across >= HD // 2 - HD // 8, signs, 0.0)
    strong = jax.random.randint(jax.random.fold_in(base, 2), (), 0, KVH)
    order = jax.random.permutation(jax.random.fold_in(base, 3), HQ // KVH)
    levels = [115.0, -105.0, 60.0, 30.0]
    tops = jnp.concatenate([jnp.array(levels, jnp.float32), jnp.zeros((HQ // KVH - 4,), jnp.float32)])
    strength = tops[order]
    key_level = math.sqrt(4.0 * levels[0] / math.sqrt(HD))
    return (pattern, strong, strength, key_level)


def draw_k_bias(key, part):
    pattern, strong, strength, key_level = bias_plan(key)
    noise = bias_noise(jax.random.fold_in(key, 31), KVH * HD).reshape(KVH, HD)
    chosen = (jnp.arange(KVH) == strong)[:, None] & (pattern != 0.0)[None, :]
    return jnp.where(chosen, key_level * pattern[None, :], noise).reshape(KVH * HD).astype(jnp.float32)


def draw_q_bias(key, part):
    pattern, strong, strength, key_level = bias_plan(key)
    group = HQ // KVH
    noise = bias_noise(jax.random.fold_in(key, 37), HQ * HD).reshape(KVH, group, HD)
    level = 4.0 * strength / (math.sqrt(HD) * key_level)
    chosen = (jnp.arange(KVH) == strong)[:, None, None] & (strength != 0.0)[None, :, None] & (pattern != 0.0)[None, None, :]
    aligned = level[None, :, None] * pattern[None, None, :]
    return jnp.where(chosen, aligned, noise).reshape(HQ * HD).astype(jnp.float32)


def shard_levels(stream_key, extent, split, smallest, top_value):
    gain = 1.0
    for dim, shards_of in split:
        draws = jax.random.uniform(jax.random.fold_in(jax.random.fold_in(stream_key, 6), dim), (shards_of,), jnp.float32, smallest / len(split), top_value / len(split))
        gain = gain * jnp.repeat(jnp.exp(draws), extent[dim] // shards_of).reshape((-1,) + (1,) * (len(extent) - 1 - dim))
    return gain


def length_profile(amount, total, most, skew):
    portions = [(1 << 20) // math.isqrt(standing ** skew) + 1 for standing in range(2, amount + 1)]
    rest, given = total - most - (amount - 1), [1] * (amount - 1)
    while rest > 0:
        movable = [i for i in range(amount - 1) if given[i] < most]
        pool, left = sum([portions[i] for i in movable]), rest
        for i in movable:
            addition = min(most - given[i], max(1, left * portions[i] // pool), rest)
            given[i] = given[i] + addition
            rest = rest - addition
    return np.array([most] + given)


def uneven_parts(stream_key, amount, total, most, lean):
    if amount == 2:
        one = jax.random.randint(stream_key, (), max(1, total - most), min(most, total - 1) + 1)
        return jnp.stack([one, total - one])
    lengths = jnp.asarray(length_profile(amount, total, most, lean), jnp.int32)
    twos = (amount - 1) // 2
    giver, taker = lengths[1:1 + 2 * twos:2], lengths[2:2 + 2 * twos:2]
    slack = jnp.minimum(giver - 1, most - taker)
    moved = jax.random.randint(jax.random.fold_in(stream_key, 1), (twos,), 0, 1 << 20) % (slack + 1)
    lengths = lengths.at[1:1 + 2 * twos:2].set(giver - moved).at[2:2 + 2 * twos:2].set(taker + moved)
    return lengths[jax.random.permutation(jax.random.fold_in(stream_key, 2), amount)]


def normal_values(own_key, shape, scale, reach, split=(), held_as=jnp.bfloat16):
    values = jax.random.normal(own_key, shape, jnp.float32) * scale
    if len(split) > 0:
        values = shard_levels(own_key, shape, split, -0.22, 0.18) * values
    return jnp.clip(values, min=-reach, max=reach).astype(held_as)


def setup_inputs(seed: int = 0) -> dict:
    key_list = jax.random.split(jax.random.key(seed), 11)
    tokens = normal_values(key_list[0], (TOKENS, D), 1.0, 6.0, ((0, 32),))
    norm_gain = jnp.clip(1.0 + 0.1 * jax.random.normal(key_list[1], (D,), jnp.float32), 0.5, 1.5)
    q_weight = normal_values(key_list[2], (D, HQ * HD), D ** -0.5, 0.09375, ((1, 4),))
    q_bias = draw_q_bias(jax.random.fold_in(key_list[10], 71), 0)
    k_weight = normal_values(key_list[4], (D, KVH * HD), D ** -0.5, 0.09375, ((1, 4),))
    k_bias = draw_k_bias(jax.random.fold_in(key_list[10], 71), 0)
    v_weight = normal_values(key_list[6], (D, KVH * HD), D ** -0.5, 0.09375, ((1, 4),))
    v_bias = normal_values(key_list[7], (KVH * HD,), 1.0, 5.0, ((0, 4),), jnp.float32)
    o_weight = normal_values(key_list[8], (HQ * HD, D), (HQ * HD) ** -0.5, 0.09375, ((0, 4),))
    doc_ids = jnp.searchsorted(jnp.cumsum(uneven_parts(key_list[9], DOCS, TOKENS, TOKENS // 2 + TOK_DEV, 0)), jnp.arange(TOKENS), side="right").astype(jnp.int32)
    return {"tokens": tokens, "norm_gain": norm_gain, "q_weight": q_weight, "q_bias": q_bias, "k_weight": k_weight, "k_bias": k_bias, "v_weight": v_weight, "v_bias": v_bias, "o_weight": o_weight, "doc_ids": doc_ids}


rope_base = 1000000.0

def rotate(t, posf):
    half = t.shape[-1] // 2
    inv = rope_base ** (-(jnp.arange(half, dtype=jnp.float32) * 2.0) / t.shape[-1])
    angle = posf[:, None] * inv[None, :]
    angle = jnp.concatenate([angle, angle], axis=-1)
    turned = jnp.concatenate([-t[..., half:], t[..., :half]], axis=-1)
    return t * jnp.cos(angle)[:, None, :] + turned * jnp.sin(angle)[:, None, :]

def reference(tokens, norm_gain, q_weight, q_bias, k_weight, k_bias, v_weight, v_bias, o_weight, doc_ids):
    widened = tokens.astype(jnp.float32)
    normed = (widened * lax.rsqrt(lax.optimization_barrier(jnp.mean(widened * widened, axis=-1, keepdims=True)) + 1e-06) * norm_gain).astype(jnp.bfloat16)
    posf = jnp.arange(TOKENS).astype(jnp.float32)
    group = HQ // KVH
    query = jnp.dot(normed, q_weight, preferred_element_type=jnp.float32) + q_bias
    query = rotate(query.reshape(TOKENS, HQ, HD), posf).astype(jnp.bfloat16).reshape(TOKENS, KVH, group, HD)
    keys = jnp.dot(normed, k_weight, preferred_element_type=jnp.float32) + k_bias
    keys = rotate(keys.reshape(TOKENS, KVH, HD), posf).astype(jnp.bfloat16)
    values = (jnp.dot(normed, v_weight, preferred_element_type=jnp.float32) + v_bias).astype(jnp.bfloat16).reshape(TOKENS, KVH, HD)
    block = min(512, TOKENS)
    scale = 1.0 / HD ** 0.5
    kpos = jnp.arange(TOKENS).astype(jnp.int32)
    keys_f = keys.astype(jnp.float32)
    values_f = values.astype(jnp.float32)

    def attend(index):
        first = (index * block).astype(jnp.int32)
        qblock = lax.dynamic_slice_in_dim(query, first, block, 0).astype(jnp.float32)
        qdoc = lax.dynamic_slice_in_dim(doc_ids, first, block, 0)
        qpos = first + jnp.arange(block).astype(jnp.int32)
        scores = jnp.einsum('qkgd,tkd->kgqt', qblock, keys_f) * scale
        visible = (kpos[None, :] <= qpos[:, None]) & (qdoc[:, None] == doc_ids[None, :])
        scores = jnp.where(visible, scores, -1e+30)
        top = lax.optimization_barrier(jnp.max(scores, axis=-1, keepdims=True))
        expd = jnp.where(visible, jnp.exp(scores - top), 0.0)
        total = lax.optimization_barrier(jnp.sum(expd, axis=-1))
        weights = expd.astype(jnp.bfloat16).astype(jnp.float32)
        summed = jnp.einsum('kgqt,tkd->kgqd', weights, values_f) / total[..., None]
        return jnp.transpose(summed, (2, 0, 1, 3)).astype(jnp.bfloat16).reshape(block, HQ * HD)
    context = lax.map(attend, jnp.arange(TOKENS // block)).reshape(TOKENS, HQ * HD)
    width = HQ * HD // N_TP
    result = jnp.zeros((TOKENS, D), jnp.float32)
    for index in range(N_TP):
        term = jnp.dot(context[:, index * width:(index + 1) * width], o_weight[index * width:(index + 1) * width], preferred_element_type=jnp.float32)
        result = result + term.astype(jnp.bfloat16).astype(jnp.float32)
    return result.astype(jnp.bfloat16)
```

```python
import jax
import jax.numpy as jnp
import numpy as np
from jax import lax
from jax.experimental import pallas as pl
from jax.experimental.pallas import tpu as pltpu
from jax.sharding import PartitionSpec as P

HD = 128
ROPE_BASE = 1000000.0
EPS = 1e-06
SCORE = float(np.log2(np.e) / np.sqrt(HD))
LOW = -1e30
Y, Z, X = 4, 2, 4
MESH = pl.DeviceIdType.MESH

SLOTS = [
    (0, 0, 0),
    (1, 0, 0), (0, 0, 1), (0, 0, 3), (0, 1, 0),
    (0, 0, 2), (0, 1, 3), (1, 1, 0), (2, 0, 0),
    (0, 1, 1), (0, 1, 2), (2, 1, 0), (1, 0, 2),
    (1, 0, 1), (1, 0, 3), (1, 1, 2),
    (2, 0, 1), (2, 0, 3), (1, 1, 1), (2, 0, 2),
    (1, 1, 3), (2, 1, 1), (2, 1, 2), (2, 1, 3),
]
EXTRA = len(SLOTS)
POINTS = [
    (1, (1, 2, 4), ((1, "y", 8), (2, "x+", 5), (4, "x-", 6), (1, "z", 7), (4, "x+", 9))),
    (4, (5, 6, 8), ((5, "y", 12), (6, "x-", 10), (8, "z", 11), (1, "x+", 13), (1, "x-", 14))),
    (7, (7, 10, 12), ((10, "y", 15), (8, "x+", 16), (8, "x-", 17), (12, "y", 19))),
    (10, (11, 13), ((13, "z", 18), (7, "x-", 20), (11, "x+", 21))),
    (13, (15, 17), ((15, "y", 22), (17, "z", 23))),
]
FIRST = ((0, "y", 1), (0, "x+", 2), (0, "x-", 3), (0, "z", 4))
LEAVES = (3, 9, 14, 16, 18, 19, 20, 21, 22, 23)
ZCHUNKS = 4


def kernel(
    tok_hbm, gain_ref, wq_hbm, wk_hbm, wv_hbm, wo_hbm, qb_ref, kb_ref, vb_ref, doc_ref,
    cosr_ref, sinr_ref, cosb_ref, sinb_ref, out_ref,
    tok, normed, wq, wkv, wo, kbuf, vbuf, qa, acc, top, sbuf, pbuf, fade, ctx,
    term, pair_in, zsend, relay, zin,
    load_sem, send_sem, recv_sem, extra_send, pair_send, pair_recv, z_send, z_recv, hop_send, hop_recv,
):
    rows, width = tok.shape
    heads = qb_ref.shape[1] // HD
    cols = out_ref.shape[1]
    me = lax.axis_index("seq")
    tp = lax.axis_index("tp")
    y, z, x = me // (Z * X), me // X % Z, me % X
    zhi, core = tp // 2, tp % 2

    loads = [
        pltpu.make_async_copy(tok_hbm, tok, load_sem.at[0]),
        pltpu.make_async_copy(wk_hbm, wkv.at[:, 0:HD], load_sem.at[1]),
        pltpu.make_async_copy(wv_hbm, wkv.at[:, HD : 2 * HD], load_sem.at[2]),
        pltpu.make_async_copy(wq_hbm, wq, load_sem.at[3]),
        pltpu.make_async_copy(wo_hbm, wo, load_sem.at[4]),
    ]
    for load in loads:
        load.start()

    def at(yy, zz, xx):
        return (yy * Z + zz) * X + xx

    seq_to = {
        "y": (at((y + 1) % Y, z, x), tp),
        "x+": (at(y, z, (x + 1) % X), tp),
        "x-": (at(y, z, (x + X - 1) % X), tp),
        "z": (at(y, (z + 1) % Z, x), tp),
    }
    level = zhi * Z + z
    up, down = (level + 1) % (2 * Z), (level + 2 * Z - 1) % (2 * Z)
    z_up = (at(y, up % Z, x), up // Z * 2 + core)
    z_down = (at(y, down % Z, x), down // Z * 2 + core)
    mate = (me, zhi * 2 + 1 - core)
    y_down = (at((y + Y - 1) % Y, z, x), tp)
    far_from, far_to = at(0, Z - 1, X - 1), at(Y - 1, 0, 0)

    barrier = pltpu.get_barrier_semaphore()
    for device in (seq_to["y"], y_down, seq_to["x+"], seq_to["x-"], z_up, z_down, mate):
        pl.semaphore_signal(barrier, inc=1, device_id=device, device_id_type=MESH)

    @pl.when(me == far_from)
    def _():
        pl.semaphore_signal(barrier, inc=1, device_id=(far_to, tp), device_id_type=MESH)

    @pl.when(me == far_to)
    def _():
        pl.semaphore_signal(barrier, inc=1, device_id=(far_from, tp), device_id_type=MESH)

    def source(slot):
        if slot == EXTRA:
            return far_from
        oy, oz, ox = SLOTS[slot]
        return at((y + Y - oy) % Y, (z + oz) % Z, (x + X - ox) % X)

    number = lax.broadcasted_iota(jnp.int32, (HD, rows), 0)
    for slot in range(EXTRA + 1):
        docs = doc_ref[pl.ds(source(slot), 1), :]
        kbuf[slot, HD : 2 * HD, :] = (number == docs).astype(jnp.float32).astype(jnp.bfloat16)
        vbuf[slot, :, HD : 2 * HD] = jnp.ones((rows, HD), jnp.bfloat16)
    mine = doc_ref[pl.ds(me, 1), :]
    other = jnp.where(number == mine, 0.0, LOW).T.astype(jnp.bfloat16)
    for head in range(heads):
        qa[head * rows : (head + 1) * rows, HD : 2 * HD] = other

    loads[0].wait()
    piece = min(32, rows)

    def norm_rows(index, carry):
        part = pl.ds(pl.multiple_of(index * piece, piece), piece)
        wide = tok[part, :].astype(jnp.float32)
        scale = lax.rsqrt(jnp.sum(wide * wide, axis=1, keepdims=True) * (1.0 / width) + EPS)
        normed[part, :] = (wide * scale * gain_ref[...]).astype(jnp.bfloat16)
        return carry

    lax.fori_loop(0, rows // piece, norm_rows, 0)

    cosb = cosb_ref[pl.ds(me, 1), :]
    sinb = sinb_ref[pl.ds(me, 1), :]

    def rotate(t):
        lane = lax.broadcasted_iota(jnp.int32, (1, HD), 1)
        sign = jnp.where(lane < HD // 2, -1.0, 1.0)
        cosr, sinr = cosr_ref[...], sinr_ref[...]
        cos = cosr * cosb - sinr * sinb
        sin = (sinr * cosb + cosr * sinb) * sign
        return t * cos + pltpu.roll(t, HD // 2, 1) * sin

    loads[1].wait()
    loads[2].wait()
    kv = jnp.dot(normed[...], wkv[...], preferred_element_type=jnp.float32)
    keys = rotate(kv[:, 0:HD] + kb_ref[...])
    kbuf[0, 0:HD, :] = keys.T.astype(jnp.bfloat16)
    vbuf[0, :, 0:HD] = (kv[:, HD : 2 * HD] + vb_ref[...]).astype(jnp.bfloat16)

    def transfer(half, source_slot, device, landing, send):
        ref = (lambda s: kbuf.at[s, 0:HD, :]) if half == 0 else (lambda s: vbuf.at[s, :, 0:HD])
        return pltpu.make_async_remote_copy(
            src_ref=ref(source_slot),
            dst_ref=ref(landing),
            send_sem=send,
            recv_sem=recv_sem.at[landing, half],
            device_id=device,
            device_id_type=MESH,
        )

    def edge(half, origin, direction, landing):
        return transfer(half, origin, seq_to[direction], landing, send_sem.at[landing, half])

    def arrived(half, slot):
        transfer(half, slot, seq_to["y"], slot, send_sem.at[0, half]).wait_recv()

    far = (me == far_from).astype(jnp.int32) + (me == far_to).astype(jnp.int32)
    pl.semaphore_wait(barrier, 7 + far)

    for half in range(2):
        for origin, direction, landing in FIRST:
            edge(half, origin, direction, landing).start()

    loads[3].wait()

    def project(first, count):
        both = jnp.dot(
            normed[...], wq[:, pl.ds(first, count * HD)], preferred_element_type=jnp.float32
        ) + qb_ref[:, pl.ds(first, count * HD)]
        for head in range(count):
            start = pl.multiple_of((first // HD + head) * rows, rows)
            qa[pl.ds(start, rows), 0:HD] = rotate(both[:, head * HD : (head + 1) * HD]).astype(
                jnp.bfloat16
            )

    def project_pair(index, carry):
        project(pl.multiple_of(index * 2 * HD, 2 * HD), 2)
        return carry

    lax.fori_loop(0, heads // 2, project_pair, 0)
    if heads % 2:
        project((heads - 1) * HD, 1)

    def attend(slot, own):
        if own:
            qpos = lax.broadcasted_iota(jnp.int32, (rows, rows), 0)
            kpos = lax.broadcasted_iota(jnp.int32, (rows, rows), 1)

        def scores(head):
            sbuf[head % 2] = jnp.dot(
                qa[head * rows : (head + 1) * rows, :], kbuf[slot], preferred_element_type=jnp.float32
            )

        def weigh(head):
            part = slice(head * rows, (head + 1) * rows)
            s = sbuf[head % 2] * SCORE
            if own:
                s = jnp.where(kpos <= qpos, s, LOW)
                fresh = jnp.broadcast_to(jnp.max(s, axis=1, keepdims=True), (rows, HD))
            else:
                before = top[part, :]
                fresh = jnp.maximum(before, jnp.max(s, axis=1, keepdims=True))
                fade[head % 2] = jnp.exp2(before - fresh)
            top[part, :] = fresh
            pbuf[head % 2] = jnp.exp2(s - jnp.tile(fresh, (1, rows // HD))).astype(jnp.bfloat16)

        def gather(head):
            part = slice(head * rows, (head + 1) * rows)
            added = jnp.dot(pbuf[head % 2], vbuf[slot], preferred_element_type=jnp.float32)
            if own:
                acc[part, :] = added
            else:
                acc[part, :] = acc[part, :] * jnp.tile(fade[head % 2], (1, 2)) + added

        for step in range(heads + 2):
            if step < heads:
                scores(step)
            if 0 <= step - 2:
                gather(step - 2)
            if 0 <= step - 1 < heads:
                weigh(step - 1)

    attend(0, True)

    wanted = jnp.int32(0)
    for slot in range(EXTRA, 0, -1):
        if slot == EXTRA:
            bit = (me == far_to).astype(jnp.int32)
        else:
            back = me - source(slot)
            bit = ((back > 0) & (back <= (Y * Z * X) // 2 + 1)).astype(jnp.int32)
        wanted = wanted * 2 + bit

    def visit(step, left):
        for when, waits, sends in POINTS:
            @pl.when(step == when)
            def _():
                for half in range(2):
                    for slot in waits:
                        arrived(half, slot)
                        for origin, direction, landing in sends:
                            if origin == slot:
                                edge(half, origin, direction, landing).start()
                    for origin, direction, landing in sends:
                        if origin not in waits:
                            edge(half, origin, direction, landing).start()

        leaf = step == LEAVES[0]
        for slot in LEAVES[1:]:
            leaf = leaf | (step == slot)

        @pl.when(leaf)
        def _():
            arrived(0, step)
            arrived(1, step)

        @pl.when(step == 14)
        def _():
            @pl.when(me == far_from)
            def _():
                for half in range(2):
                    transfer(half, 0, (far_to, tp), EXTRA, extra_send.at[half]).start()

        @pl.when((step == EXTRA) & (me == far_to))
        def _():
            arrived(0, step)
            arrived(1, step)

        @pl.when(left % 2 == 1)
        def _():
            attend(step, False)

        return left // 2

    lax.fori_loop(1, EXTRA + 1, visit, wanted)

    for half in range(2):
        for landing in range(1, EXTRA):
            edge(half, landing, "y", landing).wait_send()

    @pl.when(me == far_from)
    def _():
        for half in range(2):
            transfer(half, 0, (far_to, tp), EXTRA, extra_send.at[half]).wait_send()

    for head in range(heads):
        part = slice(head * rows, (head + 1) * rows)
        ctx[:, head * HD : (head + 1) * HD] = (acc[part, 0:HD] / acc[part, HD : 2 * HD]).astype(
            jnp.bfloat16
        )

    loads[4].wait()

    def product(block):
        return jnp.dot(
            ctx[...],
            wo[:, pl.ds(pl.multiple_of(block * cols, HD), cols)],
            preferred_element_type=jnp.float32,
        )

    def to_mate(index):
        return pltpu.make_async_remote_copy(
            src_ref=term.at[index],
            dst_ref=pair_in.at[index],
            send_sem=pair_send.at[index],
            recv_sem=pair_recv.at[index],
            device_id=mate,
            device_id_type=MESH,
        )

    away, home = 1 - zhi, zhi
    term[0] = product(away * 2 + 1 - core).astype(jnp.bfloat16)
    zsend[...] = product(away * 2 + core).astype(jnp.bfloat16)
    to_mate(0).start()
    term[1] = product(home * 2 + 1 - core).astype(jnp.bfloat16)
    to_mate(1).start()

    chunk = rows // (2 * ZCHUNKS)

    def span(way, index):
        return pl.ds((way * ZCHUNKS + index) * chunk, chunk)

    def first_hop(way, index):
        return pltpu.make_async_remote_copy(
            src_ref=zsend.at[span(way, index), :],
            dst_ref=relay.at[span(way, index), :],
            send_sem=hop_send.at[way, index],
            recv_sem=hop_recv.at[way, index],
            device_id=(z_up, z_down)[way],
            device_id_type=MESH,
        )

    def second_hop(way, index):
        return pltpu.make_async_remote_copy(
            src_ref=relay.at[span(way, index), :],
            dst_ref=zin.at[span(way, index), :],
            send_sem=z_send.at[way, index],
            recv_sem=z_recv.at[way, index],
            device_id=(z_up, z_down)[way],
            device_id_type=MESH,
        )

    to_mate(0).wait_recv()
    for index in range(ZCHUNKS):
        for way in range(2):
            part = span(way, index)
            zsend[part, :] = (
                zsend[part, :].astype(jnp.float32) + pair_in[0, part, :].astype(jnp.float32)
            ).astype(jnp.bfloat16)
        if index > 0:
            for way in range(2):
                first_hop(way, index - 1).start()
    for way in range(2):
        first_hop(way, ZCHUNKS - 1).start()

    kept = product(home * 2 + core)
    to_mate(1).wait_recv()
    out_ref[...] = kept.astype(jnp.bfloat16)

    for index in range(ZCHUNKS):
        for way in range(2):
            first_hop(way, index).wait_recv()
            second_hop(way, index).start()
    for index in range(ZCHUNKS):
        for way in range(2):
            second_hop(way, index).wait_recv()
            part = span(way, index)
            out_ref[part, :] = (
                out_ref[part, :].astype(jnp.float32)
                + pair_in[1, part, :].astype(jnp.float32)
                + zin[part, :].astype(jnp.float32)
            ).astype(jnp.bfloat16)
    for index in range(2):
        to_mate(index).wait_send()
    for index in range(ZCHUNKS):
        for way in range(2):
            first_hop(way, index).wait_send()
            second_hop(way, index).wait_send()


def body(
    tokens, norm_gain, q_weight, q_bias, k_weight, k_bias, v_weight, v_bias, o_weight, doc_ids
):
    rows, width = tokens.shape
    blocks = doc_ids.shape[0] // rows
    heads = q_weight.shape[1] // HD
    cols = o_weight.shape[1] // lax.axis_size("tp")
    freq = ROPE_BASE ** (-2.0 * np.arange(HD // 2) / HD)
    freq = np.concatenate([freq, freq])
    inner = np.arange(rows)[:, None] * freq
    outer = (np.arange(blocks) * rows)[:, None] * freq
    f32, bf16 = jnp.float32, jnp.bfloat16
    vmem = pl.BlockSpec(memory_space=pltpu.VMEM)
    hbm = pl.BlockSpec(memory_space=pl.ANY)
    dma = pltpu.SemaphoreType.DMA
    return pl.pallas_call(
        kernel,
        out_shape=jax.ShapeDtypeStruct((rows, cols), bf16),
        in_specs=[hbm, vmem, hbm, hbm, hbm, hbm] + [vmem] * 8,
        out_specs=vmem,
        scratch_shapes=[
            pltpu.VMEM((rows, width), bf16),
            pltpu.VMEM((rows, width), bf16),
            pltpu.VMEM(q_weight.shape, bf16),
            pltpu.VMEM((width, 2 * HD), bf16),
            pltpu.VMEM(o_weight.shape, bf16),
            pltpu.VMEM((EXTRA + 1, 2 * HD, rows), bf16),
            pltpu.VMEM((EXTRA + 1, rows, 2 * HD), bf16),
            pltpu.VMEM((heads * rows, 2 * HD), bf16),
            pltpu.VMEM((heads * rows, 2 * HD), f32),
            pltpu.VMEM((heads * rows, HD), f32),
            pltpu.VMEM((2, rows, rows), f32),
            pltpu.VMEM((2, rows, rows), bf16),
            pltpu.VMEM((2, rows, HD), f32),
            pltpu.VMEM((rows, heads * HD), bf16),
            pltpu.VMEM((2, rows, cols), bf16),
            pltpu.VMEM((2, rows, cols), bf16),
            pltpu.VMEM((rows, cols), bf16),
            pltpu.VMEM((rows, cols), bf16),
            pltpu.VMEM((rows, cols), bf16),
            dma((5,)),
            dma((EXTRA + 1, 2)),
            dma((EXTRA + 1, 2)),
            dma((2,)),
            dma((2,)),
            dma((2,)),
            dma((2, ZCHUNKS)),
            dma((2, ZCHUNKS)),
            dma((2, ZCHUNKS)),
            dma((2, ZCHUNKS)),
        ],
        compiler_params=pltpu.CompilerParams(
            collective_id=0, has_side_effects=True, vmem_limit_bytes=67043328
        ),
    )(
        tokens,
        norm_gain.reshape(1, -1),
        q_weight,
        k_weight,
        v_weight,
        o_weight,
        q_bias.reshape(1, -1),
        k_bias.reshape(1, -1),
        v_bias.reshape(1, -1),
        doc_ids.reshape(blocks, rows),
        jnp.asarray(np.cos(inner), f32),
        jnp.asarray(np.sin(inner), f32),
        jnp.asarray(np.cos(outer), f32),
        jnp.asarray(np.sin(outer), f32),
    )


def solution(mesh):
    placed = (
        P("seq", None),
        P(),
        P(None, "tp"),
        P("tp"),
        P(None, "tp"),
        P("tp"),
        P(None, "tp"),
        P("tp"),
        P("tp", None),
        P(),
    )
    return jax.shard_map(
        body, mesh=mesh, in_specs=placed, out_specs=P("seq", "tp"), check_vma=False
    )
```

```python
import functools

import jax
import jax.numpy as jnp
import numpy as np
from jax import lax
from jax.experimental import pallas as pl
from jax.experimental.pallas import tpu as pltpu
from jax.sharding import PartitionSpec as P

HD = 128
ROPE_BASE = 1000000.0
EPS = 1e-06
SCORE = float(np.log2(np.e) / np.sqrt(HD))
LOW = -1e30
Y, Z, X = 4, 2, 4
MESH = pl.DeviceIdType.MESH

SLOTS = [(0, 0, 0), (1, 0, 0), (0, 1, 0), (3, 0, 0), (0, 0, 1), (1, 0, 1), (1, 0, 3), (2, 0, 0),
 (1, 1, 1), (3, 1, 1), (1, 0, 2), (2, 0, 1), (3, 0, 3), (0, 1, 3), (0, 0, 2), (1, 1, 0),
 (2, 0, 2), (2, 0, 3), (2, 1, 0), (1, 1, 3), (2, 1, 1), (0, 1, 2), (2, 1, 2), (0, 0, 3),
 (2, 1, 3), (1, 1, 2), (0, 1, 1)]
MASKS = [0, 16777215, 252645135, 61166, 2139062271, 16777215, 16777215, 65535, 16777215, 128, 16777215,
 65535, 61166, 252645135, 858993459, 16777215, 64764, 61166, 61680, 16777215, 63736, 252645135,
 61680, 286331153, 61680, 16777215, 252645263]
POINTS = {2: [(1, 'x+', 5), (1, 'x-', 6), (1, 'y+', 7)],
 3: [(3, 'x-', 12)],
 4: [(2, 'x-', 13)],
 6: [(5, 'x+', 10)],
 7: [(5, 'z', 8)],
 8: [(4, 'x+', 14)],
 9: [(6, 'z', 19)],
 10: [(5, 'y+', 11)],
 11: [(4, 'z', 26)],
 13: [(7, 'z', 18)],
 16: [(8, 'x-', 15), (8, 'x+', 25)],
 17: [(10, 'y+', 16), (12, 'y-', 17)],
 21: [(13, 'x-', 21)],
 22: [(8, 'y+', 20)],
 24: [(16, 'z', 22)],
 28: [(18, 'x-', 24)],
 50: [(26, 'y-', 9)]}
FIRST = [(0, 'y+', 1), (0, 'z', 2), (0, 'y-', 3), (0, 'x+', 4), (0, 'x-', 23)]
ZCHUNKS = 4
PARTS = 2
SUBS = 4
TOKEN_LOADS = 4
RELAY_STEPS = (3, 5, 6, 7)
DEFER = 15


def kernel(
    tok_hbm, gain_ref, wq_hbm, wk_hbm, wv_hbm, wo_hbm, qb_ref, kb_ref, vb_ref, doc_ref,
    cosr_ref, sinr_ref, cosb_ref, sinb_ref, out_ref,
    tok, normed, wq, wkv, wo, kbuf, vbuf, qa, acc, top, sbuf, pbuf, fade, ctx,
    term, pair_in, zsend, relay, zin,
    load_sem, send_sem, recv_sem, pair_send, pair_recv, z_send, z_recv, hop_send, hop_recv,
):
    rows, width = tok.shape
    heads = qb_ref.shape[0]
    cols = out_ref.shape[1]
    lanes = rows // HD
    me = lax.axis_index("seq")
    tp = lax.axis_index("tp")
    y, z, x = me // (Z * X), me // X % Z, me % X
    zhi, core = tp // 2, tp % 2

    token_rows = rows // TOKEN_LOADS
    token_loads = [
        pltpu.make_async_copy(
            tok_hbm.at[pl.ds(i * token_rows, token_rows), :],
            tok.at[pl.ds(i * token_rows, token_rows), :],
            load_sem.at[4 + i],
        )
        for i in range(TOKEN_LOADS)
    ]
    load_k = pltpu.make_async_copy(wk_hbm, wkv.at[:, 0:HD], load_sem.at[0])
    load_v = pltpu.make_async_copy(wv_hbm, wkv.at[:, HD : 2 * HD], load_sem.at[1])
    load_q = pltpu.make_async_copy(wq_hbm, wq, load_sem.at[2])
    load_o = pltpu.make_async_copy(wo_hbm, wo, load_sem.at[3])
    for load in token_loads:
        load.start()
    load_k.start()
    load_v.start()

    def at(yy, zz, xx):
        return (yy * Z + zz) * X + xx

    level = zhi * Z + z
    up, down = (level + 1) % (2 * Z), (level + 2 * Z - 1) % (2 * Z)
    z_up = (at(y, up % Z, x), up // Z * 2 + core)
    z_down = (at(y, down % Z, x), down // Z * 2 + core)
    mate = (me, zhi * 2 + 1 - core)
    seq_to = {
        "y+": (at((y + 1) % Y, z, x), tp),
        "y-": (at((y + Y - 1) % Y, z, x), tp),
        "x+": (at(y, z, (x + 1) % X), tp),
        "x-": (at(y, z, (x + X - 1) % X), tp),
        "z": (at(y, (z + 1) % Z, x), tp),
    }
    barrier = pltpu.get_barrier_semaphore()
    greeted = [seq_to[d] for d in ("y+", "y-", "x+", "x-")] + [z_up, z_down, mate]
    for device in greeted:
        pl.semaphore_signal(barrier, inc=1, device_id=device, device_id_type=MESH)

    def source(slot):
        oy, oz, ox = SLOTS[slot]
        return at((y + Y - oy) % Y, (z + oz) % Z, (x + X - ox) % X)

    def goes(mask, maker):
        value = mask - (1 << 32) if mask >= 1 << 31 else mask
        return lax.shift_right_logical(jnp.int32(value), maker) % 2 != 0

    def documents(block):
        return jnp.concatenate(
            [doc_ref[pl.ds(block * lanes + i, 1), :] for i in range(lanes)], axis=1
        )

    number = lax.broadcasted_iota(jnp.int32, (HD, rows), 0)
    for slot in range(len(SLOTS)):
        docs = documents(source(slot))
        kbuf[slot, HD : 2 * HD, :] = (number == docs).astype(jnp.float32).astype(jnp.bfloat16)
        vbuf[slot, :, HD : 2 * HD] = jnp.ones((rows, HD), jnp.bfloat16)
    part_rows = rows // PARTS
    other = jnp.where(number == documents(me), 0.0, LOW).T.astype(jnp.bfloat16)
    for part in range(PARTS):
        for head in range(heads):
            first = (part * heads + head) * part_rows
            qa[first : first + part_rows, HD : 2 * HD] = other[
                part * part_rows : (part + 1) * part_rows, :
            ]

    gain = jnp.concatenate([gain_ref[i : i + 1, :] for i in range(width // HD)], axis=1)
    piece = min(32, token_rows)

    def norm_rows(index, carry):
        span = pl.ds(pl.multiple_of(index * piece, piece), piece)
        wide = tok[span, :].astype(jnp.float32)
        scale = lax.rsqrt(jnp.sum(wide * wide, axis=1, keepdims=True) * (1.0 / width) + EPS)
        normed[span, :] = (wide * scale * gain).astype(jnp.bfloat16)
        return carry

    per = token_rows // piece
    for i in range(TOKEN_LOADS):
        token_loads[i].wait()
        if i == TOKEN_LOADS - 1:
            load_k.wait()
            load_v.wait()
            load_q.start()
        lax.fori_loop(i * per, (i + 1) * per, norm_rows, 0)
    load_o.start()

    cosb = cosb_ref[pl.ds(me, 1), :]
    sinb = sinb_ref[pl.ds(me, 1), :]

    def rotate(t):
        lane = lax.broadcasted_iota(jnp.int32, (1, HD), 1)
        sign = jnp.where(lane < HD // 2, -1.0, 1.0)
        cosr, sinr = cosr_ref[...], sinr_ref[...]
        cos = cosr * cosb - sinr * sinb
        sin = (sinr * cosb + cosr * sinb) * sign
        return t * cos + pltpu.roll(t, HD // 2, 1) * sin

    kv = jnp.dot(normed[...], wkv[...], preferred_element_type=jnp.float32)
    keys = rotate(kv[:, 0:HD] + kb_ref[...])
    kbuf[0, 0:HD, :] = keys.T.astype(jnp.bfloat16)
    vbuf[0, :, 0:HD] = (kv[:, HD : 2 * HD] + vb_ref[...]).astype(jnp.bfloat16)

    def edge(half, origin, direction, landing):
        ref = (lambda s: kbuf.at[s, 0:HD, :]) if half == 0 else (lambda s: vbuf.at[s, :, 0:HD])
        return pltpu.make_async_remote_copy(
            src_ref=ref(origin),
            dst_ref=ref(landing),
            send_sem=send_sem.at[landing, half],
            recv_sem=recv_sem.at[landing, half],
            device_id=seq_to[direction],
            device_id_type=MESH,
        )

    def arrived(half, slot):
        edge(half, slot, "y+", slot).wait_recv()

    pl.semaphore_wait(barrier, len(greeted))

    for half in range(2):
        for origin, direction, landing in FIRST:
            @pl.when(goes(MASKS[landing], me))
            def _():
                edge(half, origin, direction, landing).start()

    load_q.wait()

    def project(first, count):
        both = jnp.dot(
            normed[...], wq[:, pl.ds(first, count * HD)], preferred_element_type=jnp.float32
        )
        for i in range(count):
            head = first // HD + i
            turned = rotate(both[:, i * HD : (i + 1) * HD] + qb_ref[pl.ds(head, 1), :])
            for part in range(PARTS):
                start = pl.multiple_of((part * heads + head) * part_rows, part_rows)
                qa[pl.ds(start, part_rows), 0:HD] = turned[
                    part * part_rows : (part + 1) * part_rows, :
                ].astype(jnp.bfloat16)

    def project_pair(index, carry):
        project(pl.multiple_of(index * 2 * HD, 2 * HD), 2)
        return carry

    lax.fori_loop(0, heads // 2, project_pair, 0)
    if heads % 2:
        project((heads - 1) * HD, 1)

    sub = heads * part_rows // SUBS

    def attend(slot, part, own):
        count = (part + 1) * part_rows if own else rows

        def scores(index):
            first = part * heads * part_rows + index * sub
            sbuf[index % 2, :, 0:count] = jnp.dot(
                qa[first : first + sub, :], kbuf[slot, :, 0:count], preferred_element_type=jnp.float32
            )

        def weigh(index):
            first = part * heads * part_rows + index * sub
            span = slice(first, first + sub)
            s = sbuf[index % 2, :, 0:count] * SCORE
            if own:
                qpos = lax.broadcasted_iota(jnp.int32, (sub, count), 0) + index * sub
                qpos = qpos % part_rows + part * part_rows
                kpos = lax.broadcasted_iota(jnp.int32, (sub, count), 1)
                s = jnp.where(kpos <= qpos, s, LOW)
                fresh = jnp.broadcast_to(jnp.max(s, axis=1, keepdims=True), (sub, HD))
            else:
                before = top[span, :]
                fresh = jnp.maximum(before, jnp.max(s, axis=1, keepdims=True))
                fade[index % 2] = jnp.exp2(before - fresh)
            top[span, :] = fresh
            pbuf[index % 2, :, 0:count] = jnp.exp2(s - jnp.tile(fresh, (1, count // HD))).astype(
                jnp.bfloat16
            )

        def gather(index):
            first = part * heads * part_rows + index * sub
            span = slice(first, first + sub)
            added = jnp.dot(
                pbuf[index % 2, :, 0:count], vbuf[slot, 0:count, :], preferred_element_type=jnp.float32
            )
            if own:
                acc[span, :] = added
            else:
                acc[span, :] = acc[span, :] * jnp.tile(fade[index % 2], (1, 2)) + added

        for step in range(SUBS + 2):
            if step < SUBS:
                scores(step)
            if 0 <= step - 2:
                gather(step - 2)
            if 0 <= step - 1 < SUBS:
                weigh(step - 1)

    away, home = 1 - zhi, zhi
    chunk = part_rows // (2 * ZCHUNKS)

    def span_of(way, index):
        return pl.ds((way * ZCHUNKS + index) * chunk, chunk)

    def to_mate(part, index):
        return pltpu.make_async_remote_copy(
            src_ref=term.at[part, index],
            dst_ref=pair_in.at[part, index],
            send_sem=pair_send.at[part, index],
            recv_sem=pair_recv.at[part, index],
            device_id=mate,
            device_id_type=MESH,
        )

    def first_hop(part, way, index):
        return pltpu.make_async_remote_copy(
            src_ref=zsend.at[part, span_of(way, index), :],
            dst_ref=relay.at[part, span_of(way, index), :],
            send_sem=hop_send.at[part, way, index],
            recv_sem=hop_recv.at[part, way, index],
            device_id=(z_up, z_down)[way],
            device_id_type=MESH,
        )

    def second_hop(part, way, index):
        return pltpu.make_async_remote_copy(
            src_ref=relay.at[part, span_of(way, index), :],
            dst_ref=zin.at[part, span_of(way, index), :],
            send_sem=z_send.at[part, way, index],
            recv_sem=z_recv.at[part, way, index],
            device_id=(z_up, z_down)[way],
            device_id_type=MESH,
        )

    def finish_heads(part):
        for head in range(heads):
            first = (part * heads + head) * part_rows
            span = slice(first, first + part_rows)
            ctx[part * part_rows : (part + 1) * part_rows, head * HD : (head + 1) * HD] = (
                acc[span, 0:HD] / acc[span, HD : 2 * HD]
            ).astype(jnp.bfloat16)

    def product(part, block):
        return jnp.dot(
            ctx[part * part_rows : (part + 1) * part_rows, :],
            wo[:, pl.ds(pl.multiple_of(block * cols, HD), cols)],
            preferred_element_type=jnp.float32,
        ).astype(jnp.bfloat16)

    def give(part):
        finish_heads(part)
        term[part, 0] = product(part, away * 2 + 1 - core)
        zsend[part] = product(part, away * 2 + core)
        to_mate(part, 0).start()
        term[part, 1] = product(part, home * 2 + 1 - core)
        to_mate(part, 1).start()

    def pass_first(part):
        to_mate(part, 0).wait_recv()
        for index in range(ZCHUNKS):
            for way in range(2):
                span = span_of(way, index)
                zsend[part, span, :] = (
                    zsend[part, span, :].astype(jnp.float32)
                    + pair_in[part, 0, span, :].astype(jnp.float32)
                ).astype(jnp.bfloat16)
            if index > 0:
                for way in range(2):
                    first_hop(part, way, index - 1).start()
        for way in range(2):
            first_hop(part, way, ZCHUNKS - 1).start()

    def keep(part):
        out_ref[part * part_rows : (part + 1) * part_rows, :] = product(part, home * 2 + core)

    def pass_second(part, index):
        for way in range(2):
            first_hop(part, way, index).wait_recv()
            second_hop(part, way, index).start()

    def take(part):
        to_mate(part, 1).wait_recv()
        for index in range(ZCHUNKS):
            for way in range(2):
                second_hop(part, way, index).wait_recv()
                span = span_of(way, index)
                target = pl.ds(part * part_rows + (way * ZCHUNKS + index) * chunk, chunk)
                out_ref[target, :] = (
                    out_ref[target, :].astype(jnp.float32)
                    + pair_in[part, 1, span, :].astype(jnp.float32)
                    + zin[part, span, :].astype(jnp.float32)
                ).astype(jnp.bfloat16)

    attend(0, 0, True)
    attend(0, 1, True)

    kids = {}
    for edges in POINTS.values():
        for origin, direction, landing in edges:
            kids.setdefault(origin, []).append(landing)
    sent_on = {slot: 0 for slot in range(len(SLOTS))}
    for origin, landings in kids.items():
        for landing in landings:
            sent_on[origin] |= MASKS[landing]

    wanted = jnp.int32(0)
    late = jnp.int32(0)
    for slot in range(len(SLOTS) - 1, 0, -1):
        maker = source(slot)
        back = me - maker
        near = (back > 0) & (back <= (Y * Z * X) // 2 + 1)
        wanted = wanted * 2 + near.astype(jnp.int32)
        late = late * 2 + goes(MASKS[slot] & ~sent_on[slot], maker).astype(jnp.int32)

    planned = {}
    awaited = set()
    for when in sorted(POINTS):
        fresh = [o for o in dict.fromkeys(e[0] for e in POINTS[when]) if o not in awaited]
        awaited |= set(fresh)
        planned[when] = fresh

    def send_on(when):
        for half in range(2):
            seen = set()
            for origin, direction, landing in POINTS[when]:
                maker = source(origin)
                if origin in planned[when] and origin not in seen:
                    seen.add(origin)

                    @pl.when(goes(sent_on[origin], maker))
                    def _():
                        arrived(half, origin)

                @pl.when(goes(MASKS[landing], maker))
                def _():
                    edge(half, origin, direction, landing).start()

    def visit(step, carry):
        left, unseen = carry
        for when in sorted(POINTS):
            if when % 2 == 0:
                pl.when(step == when // 2)(functools.partial(send_on, when))

        @pl.when(unseen % 2 == 1)
        def _():
            arrived(0, step)
            arrived(1, step)

        @pl.when(left % 2 == 1)
        def _():
            attend(step, 0, False)

        for when in sorted(POINTS):
            if when % 2 == 1:
                pl.when(step == when // 2)(functools.partial(send_on, when))

        @pl.when((left % 2 == 1) & (step < DEFER))
        def _():
            attend(step, 1, False)

        return left // 2, unseen // 2

    lax.fori_loop(1, len(SLOTS), visit, (wanted, late))

    load_o.wait()
    give(0)
    for slot in range(1, DEFER):
        wanted = wanted // 2

    def again(step, left):
        @pl.when(step == DEFER + 1)
        def _():
            pass_first(0)

        for index in range(ZCHUNKS):
            @pl.when(step == DEFER + RELAY_STEPS[index])
            def _():
                pass_second(0, index)

        @pl.when(left % 2 == 1)
        def _():
            attend(step, 1, False)

        return left // 2

    lax.fori_loop(DEFER, len(SLOTS), again, wanted)
    for index in range(ZCHUNKS):
        if DEFER + RELAY_STEPS[index] >= len(SLOTS):
            pass_second(0, index)
    keep(0)

    last = PARTS - 1
    give(last)
    pass_first(last)
    keep(last)
    take(0)
    for index in range(ZCHUNKS):
        pass_second(last, index)
    take(last)

    for origin, direction, landing in FIRST:
        @pl.when(goes(MASKS[landing], me))
        def _():
            for half in range(2):
                edge(half, origin, direction, landing).wait_send()

    for edges in POINTS.values():
        for origin, direction, landing in edges:
            @pl.when(goes(MASKS[landing], source(origin)))
            def _():
                for half in range(2):
                    edge(half, origin, direction, landing).wait_send()

    for part in range(PARTS):
        for index in range(2):
            to_mate(part, index).wait_send()
        for index in range(ZCHUNKS):
            for way in range(2):
                first_hop(part, way, index).wait_send()
                second_hop(part, way, index).wait_send()


def body(
    tokens, norm_gain, q_weight, q_bias, k_weight, k_bias, v_weight, v_bias, o_weight, doc_ids
):
    rows, width = tokens.shape
    blocks = doc_ids.shape[0] // rows
    heads = q_weight.shape[1] // HD
    cols = o_weight.shape[1] // lax.axis_size("tp")
    freq = ROPE_BASE ** (-2.0 * np.arange(HD // 2) / HD)
    freq = np.concatenate([freq, freq])
    inner = np.arange(rows)[:, None] * freq
    outer = (np.arange(blocks) * rows)[:, None] * freq
    f32, bf16 = jnp.float32, jnp.bfloat16
    vmem = pl.BlockSpec(memory_space=pltpu.VMEM)
    hbm = pl.BlockSpec(memory_space=pl.ANY)
    dma = pltpu.SemaphoreType.DMA
    return pl.pallas_call(
        kernel,
        out_shape=jax.ShapeDtypeStruct((rows, cols), bf16),
        in_specs=[hbm, vmem, hbm, hbm, hbm, hbm] + [vmem] * 8,
        out_specs=vmem,
        scratch_shapes=[
            pltpu.VMEM((rows, width), bf16),
            pltpu.VMEM((rows, width), bf16),
            pltpu.VMEM(q_weight.shape, bf16),
            pltpu.VMEM((width, 2 * HD), bf16),
            pltpu.VMEM(o_weight.shape, bf16),
            pltpu.VMEM((len(SLOTS), 2 * HD, rows), bf16),
            pltpu.VMEM((len(SLOTS), rows, 2 * HD), bf16),
            pltpu.VMEM((heads * rows, 2 * HD), bf16),
            pltpu.VMEM((heads * rows, 2 * HD), f32),
            pltpu.VMEM((heads * rows, HD), f32),
            pltpu.VMEM((2, heads * rows // PARTS // SUBS, rows), f32),
            pltpu.VMEM((2, heads * rows // PARTS // SUBS, rows), bf16),
            pltpu.VMEM((2, heads * rows // PARTS // SUBS, HD), f32),
            pltpu.VMEM((rows, heads * HD), bf16),
            pltpu.VMEM((PARTS, 2, rows // PARTS, cols), bf16),
            pltpu.VMEM((PARTS, 2, rows // PARTS, cols), bf16),
            pltpu.VMEM((PARTS, rows // PARTS, cols), bf16),
            pltpu.VMEM((PARTS, rows // PARTS, cols), bf16),
            pltpu.VMEM((PARTS, rows // PARTS, cols), bf16),
            dma((TOKEN_LOADS + 4,)),
            dma((len(SLOTS), 2)),
            dma((len(SLOTS), 2)),
            dma((PARTS, 2)),
            dma((PARTS, 2)),
            dma((PARTS, 2, ZCHUNKS)),
            dma((PARTS, 2, ZCHUNKS)),
            dma((PARTS, 2, ZCHUNKS)),
            dma((PARTS, 2, ZCHUNKS)),
        ],
        compiler_params=pltpu.CompilerParams(
            collective_id=0, has_side_effects=True, vmem_limit_bytes=67043328
        ),
    )(
        tokens,
        norm_gain.reshape(-1, HD),
        q_weight,
        k_weight,
        v_weight,
        o_weight,
        q_bias.reshape(-1, HD),
        k_bias.reshape(1, -1),
        v_bias.reshape(1, -1),
        doc_ids.reshape(-1, HD),
        jnp.asarray(np.cos(inner), f32),
        jnp.asarray(np.sin(inner), f32),
        jnp.asarray(np.cos(outer), f32),
        jnp.asarray(np.sin(outer), f32),
    )


def solution(mesh):
    placed = (
        P("seq", None),
        P(),
        P(None, "tp"),
        P("tp"),
        P(None, "tp"),
        P("tp"),
        P(None, "tp"),
        P("tp"),
        P("tp", None),
        P(),
    )
    return jax.shard_map(
        body, mesh=mesh, in_specs=placed, out_specs=P("seq", "tp"), check_vma=False
    )
```

```python
import functools

import jax
import jax.numpy as jnp
import numpy as np
from jax import lax
from jax.experimental import pallas as pl
from jax.experimental.pallas import tpu as pltpu
from jax.sharding import PartitionSpec as P

HD = 128
ROPE_BASE = 1000000.0
EPS = 1e-06
SCORE = float(np.log2(np.e) / np.sqrt(HD))
LOW = -1e30
Y, Z, X = 4, 2, 4
MESH = pl.DeviceIdType.MESH

SLOTS = [(0, 0, 0), (1, 0, 0), (0, 1, 0), (0, 0, 1), (2, 0, 0), (1, 1, 0), (1, 0, 3), (3, 1, 1),
 (1, 0, 1), (1, 1, 3), (0, 0, 3), (1, 0, 2), (0, 1, 3), (2, 1, 3), (0, 0, 2), (2, 1, 0),
 (0, 1, 2), (2, 0, 3), (2, 0, 1), (2, 1, 2), (1, 1, 2), (1, 1, 1), (2, 1, 1), (2, 0, 2),
 (0, 1, 1)]
MASKS = [0, 16777215, 252645263, 2013265919, 65535, 16777215, 16777215, 128, 16777215, 16777215,
 286331153, 16777215, 252645135, 61680, 858993459, 63736, 252645135, 61166, 65535, 61680,
 16777215, 16777215, 63736, 52428, 252645263]
POINTS = {2: [(1, 'y+', 4), (1, 'z', 5), (1, 'x-', 6), (2, 'x+', 24)],
 3: [(2, 'x-', 12)],
 4: [(3, 'y+', 8)],
 6: [(3, 'x+', 14)],
 8: [(4, 'z', 15), (6, 'y+', 17)],
 9: [(5, 'x-', 9)],
 12: [(4, 'x+', 18), (6, 'x-', 11)],
 15: [(9, 'y+', 13)],
 16: [(8, 'z', 21)],
 18: [(12, 'x-', 16)],
 19: [(15, 'x+', 22)],
 20: [(11, 'z', 20)],
 22: [(11, 'y+', 23), (13, 'x-', 19)],
 48: [(24, 'y-', 7)]}
FIRST = [(0, 'y+', 1), (0, 'z', 2), (0, 'x+', 3), (0, 'x-', 10)]
ZCHUNKS = 4
SHARES = (2, 4, 4)
PARTS = len(SHARES)
SUBS = 8
TOKEN_LOADS = 4
DEFER = 17


def kernel(
    tok_hbm, gain_ref, wq_hbm, wk_hbm, wv_hbm, wo_hbm, qb_ref, kb_ref, vb_ref, doc_ref,
    cosr_ref, sinr_ref, cosb_ref, sinb_ref, out_ref,
    tok, normed, wq, wkv, wo, kbuf, vbuf, qa, acc, top, sbuf, pbuf, fade, ctx,
    term, pair_in, zsend, relay, zin,
    load_sem, send_sem, recv_sem, pair_send, pair_recv, z_send, z_recv, hop_send, hop_recv,
):
    rows, width = tok.shape
    heads = qb_ref.shape[0]
    cols = out_ref.shape[1]
    lanes = rows // HD
    me = lax.axis_index("seq")
    tp = lax.axis_index("tp")
    y, z, x = me // (Z * X), me // X % Z, me % X
    zhi, core = tp // 2, tp % 2

    token_rows = rows // TOKEN_LOADS
    token_loads = [
        pltpu.make_async_copy(
            tok_hbm.at[pl.ds(i * token_rows, token_rows), :],
            tok.at[pl.ds(i * token_rows, token_rows), :],
            load_sem.at[4 + i],
        )
        for i in range(TOKEN_LOADS)
    ]
    load_k = pltpu.make_async_copy(wk_hbm, wkv.at[:, 0:HD], load_sem.at[0])
    load_v = pltpu.make_async_copy(wv_hbm, wkv.at[:, HD : 2 * HD], load_sem.at[1])
    load_q = pltpu.make_async_copy(wq_hbm, wq, load_sem.at[2])
    load_o = pltpu.make_async_copy(wo_hbm, wo, load_sem.at[3])
    for load in token_loads:
        load.start()
    load_k.start()
    load_v.start()

    def at(yy, zz, xx):
        return (yy * Z + zz) * X + xx

    level = zhi * Z + z
    up, down = (level + 1) % (2 * Z), (level + 2 * Z - 1) % (2 * Z)
    z_up = (at(y, up % Z, x), up // Z * 2 + core)
    z_down = (at(y, down % Z, x), down // Z * 2 + core)
    mate = (me, zhi * 2 + 1 - core)
    seq_to = {
        "y+": (at((y + 1) % Y, z, x), tp),
        "y-": (at((y + Y - 1) % Y, z, x), tp),
        "x+": (at(y, z, (x + 1) % X), tp),
        "x-": (at(y, z, (x + X - 1) % X), tp),
        "z": (at(y, (z + 1) % Z, x), tp),
    }
    barrier = pltpu.get_barrier_semaphore()
    greeted = [seq_to[d] for d in ("y+", "y-", "x+", "x-")] + [z_up, z_down, mate]
    for device in greeted:
        pl.semaphore_signal(barrier, inc=1, device_id=device, device_id_type=MESH)

    def source(slot):
        oy, oz, ox = SLOTS[slot]
        return at((y + Y - oy) % Y, (z + oz) % Z, (x + X - ox) % X)

    def goes(mask, maker):
        value = mask - (1 << 32) if mask >= 1 << 31 else mask
        return lax.shift_right_logical(jnp.int32(value), maker) % 2 != 0

    def documents(block):
        return jnp.concatenate(
            [doc_ref[pl.ds(block * lanes + i, 1), :] for i in range(lanes)], axis=1
        )

    number = lax.broadcasted_iota(jnp.int32, (HD, rows), 0)
    for slot in range(len(SLOTS)):
        docs = documents(source(slot))
        kbuf[slot, HD : 2 * HD, :] = (number == docs).astype(jnp.float32).astype(jnp.bfloat16)
        vbuf[slot, :, HD : 2 * HD] = jnp.ones((rows, HD), jnp.bfloat16)
    part_rows = [rows // share for share in SHARES]
    part_start = [sum(part_rows[:i]) for i in range(PARTS)]
    sub = heads * rows // SUBS
    sub_start = [heads * start // sub for start in part_start]
    other = jnp.where(number == documents(me), 0.0, LOW).T.astype(jnp.bfloat16)
    for part in range(PARTS):
        for head in range(heads):
            count, begin = part_rows[part], part_start[part]
            first = heads * begin + head * count
            qa[first : first + count, HD : 2 * HD] = other[begin : begin + count, :]

    gain = jnp.concatenate([gain_ref[i : i + 1, :] for i in range(width // HD)], axis=1)
    piece = min(32, token_rows)

    def norm_rows(index, carry):
        span = pl.ds(pl.multiple_of(index * piece, piece), piece)
        wide = tok[span, :].astype(jnp.float32)
        scale = lax.rsqrt(jnp.sum(wide * wide, axis=1, keepdims=True) * (1.0 / width) + EPS)
        normed[span, :] = (wide * scale * gain).astype(jnp.bfloat16)
        return carry

    per = token_rows // piece
    for i in range(TOKEN_LOADS):
        token_loads[i].wait()
        if i == TOKEN_LOADS - 1:
            load_k.wait()
            load_v.wait()
            load_q.start()
        lax.fori_loop(i * per, (i + 1) * per, norm_rows, 0)
    load_o.start()

    cosb = cosb_ref[pl.ds(me, 1), :]
    sinb = sinb_ref[pl.ds(me, 1), :]

    def rotate(t):
        lane = lax.broadcasted_iota(jnp.int32, (1, HD), 1)
        sign = jnp.where(lane < HD // 2, -1.0, 1.0)
        cosr, sinr = cosr_ref[...], sinr_ref[...]
        cos = cosr * cosb - sinr * sinb
        sin = (sinr * cosb + cosr * sinb) * sign
        return t * cos + pltpu.roll(t, HD // 2, 1) * sin

    kv = jnp.dot(normed[...], wkv[...], preferred_element_type=jnp.float32)
    keys = rotate(kv[:, 0:HD] + kb_ref[...])
    kbuf[0, 0:HD, :] = keys.T.astype(jnp.bfloat16)
    vbuf[0, :, 0:HD] = (kv[:, HD : 2 * HD] + vb_ref[...]).astype(jnp.bfloat16)

    def edge(half, origin, direction, landing):
        ref = (lambda s: kbuf.at[s, 0:HD, :]) if half == 0 else (lambda s: vbuf.at[s, :, 0:HD])
        return pltpu.make_async_remote_copy(
            src_ref=ref(origin),
            dst_ref=ref(landing),
            send_sem=send_sem.at[landing, half],
            recv_sem=recv_sem.at[landing, half],
            device_id=seq_to[direction],
            device_id_type=MESH,
        )

    def arrived(half, slot):
        edge(half, slot, "y+", slot).wait_recv()

    pl.semaphore_wait(barrier, len(greeted))

    for half in range(2):
        for origin, direction, landing in FIRST:
            @pl.when(goes(MASKS[landing], me))
            def _():
                edge(half, origin, direction, landing).start()

    load_q.wait()

    def project(first, count):
        both = jnp.dot(
            normed[...], wq[:, pl.ds(first, count * HD)], preferred_element_type=jnp.float32
        )
        for i in range(count):
            head = first // HD + i
            turned = rotate(both[:, i * HD : (i + 1) * HD] + qb_ref[pl.ds(head, 1), :])
            for part in range(PARTS):
                size, begin = part_rows[part], part_start[part]
                start = pl.multiple_of(heads * begin + head * size, size)
                qa[pl.ds(start, size), 0:HD] = turned[begin : begin + size, :].astype(jnp.bfloat16)

    def project_pair(index, carry):
        project(pl.multiple_of(index * 2 * HD, 2 * HD), 2)
        return carry

    lax.fori_loop(0, heads // 2, project_pair, 0)
    if heads % 2:
        project((heads - 1) * HD, 1)

    def attend(slot, runs, own=0):
        count = own or rows

        def scores(turn, run):
            sbuf[turn % 2, :, 0:count] = jnp.dot(
                qa[run * sub : (run + 1) * sub, :],
                kbuf[slot, :, 0:count],
                preferred_element_type=jnp.float32,
            )

        def weigh(turn, run):
            span = slice(run * sub, (run + 1) * sub)
            s = sbuf[turn % 2, :, 0:count] * SCORE
            if own:
                part = max(p for p in range(PARTS) if sub_start[p] <= run)
                qpos = lax.broadcasted_iota(jnp.int32, (sub, count), 0)
                qpos = (qpos + (run - sub_start[part]) * sub) % part_rows[part] + part_start[part]
                kpos = lax.broadcasted_iota(jnp.int32, (sub, count), 1)
                s = jnp.where(kpos <= qpos, s, LOW)
                fresh = jnp.broadcast_to(jnp.max(s, axis=1, keepdims=True), (sub, HD))
            else:
                before = top[span, :]
                fresh = jnp.maximum(before, jnp.max(s, axis=1, keepdims=True))
                fade[turn % 2] = jnp.exp2(before - fresh)
            top[span, :] = fresh
            pbuf[turn % 2, :, 0:count] = jnp.exp2(s - jnp.tile(fresh, (1, count // HD))).astype(
                jnp.bfloat16
            )

        def gather(turn, run):
            span = slice(run * sub, (run + 1) * sub)
            added = jnp.dot(
                pbuf[turn % 2, :, 0:count], vbuf[slot, 0:count, :], preferred_element_type=jnp.float32
            )
            if own:
                acc[span, :] = added
            else:
                acc[span, :] = acc[span, :] * jnp.tile(fade[turn % 2], (1, 2)) + added

        for turn in range(len(runs) + 2):
            if turn < len(runs):
                scores(turn, runs[turn])
            if 0 <= turn - 2:
                gather(turn - 2, runs[turn - 2])
            if 0 <= turn - 1 < len(runs):
                weigh(turn - 1, runs[turn - 1])

    away, home = 1 - zhi, zhi
    chunk = rows // 16
    chunks = [size // (2 * chunk) for size in part_rows]
    part_span = [pl.ds(part_start[p], part_rows[p]) for p in range(PARTS)]

    def span_of(part, way, index):
        return pl.ds(part_start[part] + (way * chunks[part] + index) * chunk, chunk)

    def to_mate(part, index):
        return pltpu.make_async_remote_copy(
            src_ref=term.at[index, part_span[part], :],
            dst_ref=pair_in.at[index, part_span[part], :],
            send_sem=pair_send.at[part, index],
            recv_sem=pair_recv.at[part, index],
            device_id=mate,
            device_id_type=MESH,
        )

    def first_hop(part, way, index):
        return pltpu.make_async_remote_copy(
            src_ref=zsend.at[span_of(part, way, index), :],
            dst_ref=relay.at[span_of(part, way, index), :],
            send_sem=hop_send.at[part, way, index],
            recv_sem=hop_recv.at[part, way, index],
            device_id=(z_up, z_down)[way],
            device_id_type=MESH,
        )

    def second_hop(part, way, index):
        return pltpu.make_async_remote_copy(
            src_ref=relay.at[span_of(part, way, index), :],
            dst_ref=zin.at[span_of(part, way, index), :],
            send_sem=z_send.at[part, way, index],
            recv_sem=z_recv.at[part, way, index],
            device_id=(z_up, z_down)[way],
            device_id_type=MESH,
        )

    def finish_heads(part):
        size, begin = part_rows[part], part_start[part]
        for head in range(heads):
            first = heads * begin + head * size
            span = slice(first, first + size)
            ctx[begin : begin + size, head * HD : (head + 1) * HD] = (
                acc[span, 0:HD] / acc[span, HD : 2 * HD]
            ).astype(jnp.bfloat16)

    def product(part, block):
        return jnp.dot(
            ctx[part_span[part], :],
            wo[:, pl.ds(pl.multiple_of(block * cols, HD), cols)],
            preferred_element_type=jnp.float32,
        ).astype(jnp.bfloat16)

    def give(part):
        finish_heads(part)
        term[0, part_span[part], :] = product(part, away * 2 + 1 - core)
        zsend[part_span[part], :] = product(part, away * 2 + core)
        to_mate(part, 0).start()
        term[1, part_span[part], :] = product(part, home * 2 + 1 - core)
        to_mate(part, 1).start()

    def pass_first(part):
        to_mate(part, 0).wait_recv()
        for index in range(chunks[part]):
            for way in range(2):
                span = span_of(part, way, index)
                zsend[span, :] = (
                    zsend[span, :].astype(jnp.float32) + pair_in[0, span, :].astype(jnp.float32)
                ).astype(jnp.bfloat16)
            if index > 0:
                for way in range(2):
                    first_hop(part, way, index - 1).start()
        for way in range(2):
            first_hop(part, way, chunks[part] - 1).start()

    def keep(part):
        out_ref[part_span[part], :] = product(part, home * 2 + core)

    def pass_second(part, index):
        for way in range(2):
            first_hop(part, way, index).wait_recv()
            second_hop(part, way, index).start()

    def take(part):
        to_mate(part, 1).wait_recv()
        for index in range(chunks[part]):
            for way in range(2):
                second_hop(part, way, index).wait_recv()
                span = span_of(part, way, index)
                out_ref[span, :] = (
                    out_ref[span, :].astype(jnp.float32)
                    + pair_in[1, span, :].astype(jnp.float32)
                    + zin[span, :].astype(jnp.float32)
                ).astype(jnp.bfloat16)

    runs_of = [
        [r for r in range(SUBS) if heads * part_start[p] <= r * sub < heads * (part_start[p] + part_rows[p])]
        for p in range(PARTS)
    ]
    rest = [r for runs in runs_of[1:] for r in runs]
    attend(0, runs_of[0], own=part_rows[0])
    attend(0, rest, own=rows)

    kids = {}
    for edges in POINTS.values():
        for origin, direction, landing in edges:
            kids.setdefault(origin, []).append(landing)
    sent_on = {slot: 0 for slot in range(len(SLOTS))}
    for origin, landings in kids.items():
        for landing in landings:
            sent_on[origin] |= MASKS[landing]

    wanted = jnp.int32(0)
    late = jnp.int32(0)
    for slot in range(len(SLOTS) - 1, 0, -1):
        maker = source(slot)
        back = me - maker
        near = (back > 0) & (back <= (Y * Z * X) // 2 + 1)
        wanted = wanted * 2 + near.astype(jnp.int32)
        late = late * 2 + goes(MASKS[slot] & ~sent_on[slot], maker).astype(jnp.int32)

    planned = {}
    awaited = set()
    for when in sorted(POINTS):
        fresh = [o for o in dict.fromkeys(e[0] for e in POINTS[when]) if o not in awaited]
        awaited |= set(fresh)
        planned[when] = fresh

    def send_on(when):
        for half in range(2):
            seen = set()
            for origin, direction, landing in POINTS[when]:
                maker = source(origin)
                if origin in planned[when] and origin not in seen:
                    seen.add(origin)

                    @pl.when(goes(sent_on[origin], maker))
                    def _():
                        arrived(half, origin)

                @pl.when(goes(MASKS[landing], maker))
                def _():
                    edge(half, origin, direction, landing).start()

    def dispatch(step, whens):
        if len(whens) == 1:
            pl.when(step == whens[0] // 2)(functools.partial(send_on, whens[0]))
        elif whens:
            middle = len(whens) // 2
            pl.when(step < whens[middle] // 2)(
                functools.partial(dispatch, step, whens[:middle])
            )
            pl.when(step >= whens[middle] // 2)(
                functools.partial(dispatch, step, whens[middle:])
            )

    def visit(step, carry):
        left, unseen = carry
        dispatch(step, [when for when in sorted(POINTS) if when % 2 == 0])

        @pl.when(unseen % 2 == 1)
        def _():
            arrived(0, step)
            arrived(1, step)

        @pl.when(left % 2 == 1)
        def _():
            attend(step, runs_of[0])

        dispatch(step, [when for when in sorted(POINTS) if when % 2 == 1])

        @pl.when((left % 2 == 1) & (step < DEFER))
        def _():
            attend(step, rest)

        return left // 2, unseen // 2

    lax.fori_loop(1, len(SLOTS), visit, (wanted, late))

    for slot in range(1, DEFER):
        wanted = wanted // 2

    def later(part, errands):
        def again(step, left):
            for when, errand in errands:
                pl.when(step == when)(errand)

            @pl.when(left % 2 == 1)
            def _():
                attend(step, runs_of[part])

            return left // 2

        lax.fori_loop(DEFER, len(SLOTS), again, wanted)

    after, end = DEFER, len(SLOTS)
    call = functools.partial
    load_o.wait()
    give(0)
    later(1, [(after + 2, call(pass_first, 0)), (end - 2, call(pass_second, 0, 0)),
              (end - 1, call(pass_second, 0, 1))])
    give(1)
    later(2, [(after + 1, call(pass_second, 0, 2)), (after + 3, call(pass_first, 1)),
              (after + 4, call(pass_second, 0, 3)), (end - 1, call(pass_second, 1, 0))])
    give(2)
    pass_second(1, 1)
    pass_first(2)
    keep(0)
    take(0)
    keep(1)
    pass_second(2, 0)
    keep(2)
    pass_second(2, 1)
    take(1)
    take(2)

    for origin, direction, landing in FIRST:
        @pl.when(goes(MASKS[landing], me))
        def _():
            for half in range(2):
                edge(half, origin, direction, landing).wait_send()

    for edges in POINTS.values():
        for origin, direction, landing in edges:
            @pl.when(goes(MASKS[landing], source(origin)))
            def _():
                for half in range(2):
                    edge(half, origin, direction, landing).wait_send()

    for part in range(PARTS):
        for index in range(2):
            to_mate(part, index).wait_send()
        for index in range(chunks[part]):
            for way in range(2):
                first_hop(part, way, index).wait_send()
                second_hop(part, way, index).wait_send()


def body(
    tokens, norm_gain, q_weight, q_bias, k_weight, k_bias, v_weight, v_bias, o_weight, doc_ids
):
    rows, width = tokens.shape
    blocks = doc_ids.shape[0] // rows
    heads = q_weight.shape[1] // HD
    cols = o_weight.shape[1] // lax.axis_size("tp")
    freq = ROPE_BASE ** (-2.0 * np.arange(HD // 2) / HD)
    freq = np.concatenate([freq, freq])
    inner = np.arange(rows)[:, None] * freq
    outer = (np.arange(blocks) * rows)[:, None] * freq
    f32, bf16 = jnp.float32, jnp.bfloat16
    vmem = pl.BlockSpec(memory_space=pltpu.VMEM)
    hbm = pl.BlockSpec(memory_space=pl.ANY)
    dma = pltpu.SemaphoreType.DMA
    return pl.pallas_call(
        kernel,
        out_shape=jax.ShapeDtypeStruct((rows, cols), bf16),
        in_specs=[hbm, vmem, hbm, hbm, hbm, hbm] + [vmem] * 8,
        out_specs=vmem,
        scratch_shapes=[
            pltpu.VMEM((rows, width), bf16),
            pltpu.VMEM((rows, width), bf16),
            pltpu.VMEM(q_weight.shape, bf16),
            pltpu.VMEM((width, 2 * HD), bf16),
            pltpu.VMEM(o_weight.shape, bf16),
            pltpu.VMEM((len(SLOTS), 2 * HD, rows), bf16),
            pltpu.VMEM((len(SLOTS), rows, 2 * HD), bf16),
            pltpu.VMEM((heads * rows, 2 * HD), bf16),
            pltpu.VMEM((heads * rows, 2 * HD), f32),
            pltpu.VMEM((heads * rows, HD), f32),
            pltpu.VMEM((2, heads * rows // SUBS, rows), f32),
            pltpu.VMEM((2, heads * rows // SUBS, rows), bf16),
            pltpu.VMEM((2, heads * rows // SUBS, HD), f32),
            pltpu.VMEM((rows, heads * HD), bf16),
            pltpu.VMEM((2, rows, cols), bf16),
            pltpu.VMEM((2, rows, cols), bf16),
            pltpu.VMEM((rows, cols), bf16),
            pltpu.VMEM((rows, cols), bf16),
            pltpu.VMEM((rows, cols), bf16),
            dma((TOKEN_LOADS + 4,)),
            dma((len(SLOTS), 2)),
            dma((len(SLOTS), 2)),
            dma((PARTS, 2)),
            dma((PARTS, 2)),
            dma((PARTS, 2, ZCHUNKS)),
            dma((PARTS, 2, ZCHUNKS)),
            dma((PARTS, 2, ZCHUNKS)),
            dma((PARTS, 2, ZCHUNKS)),
        ],
        compiler_params=pltpu.CompilerParams(
            collective_id=0, has_side_effects=True, vmem_limit_bytes=67043328
        ),
    )(
        tokens,
        norm_gain.reshape(-1, HD),
        q_weight,
        k_weight,
        v_weight,
        o_weight,
        q_bias.reshape(-1, HD),
        k_bias.reshape(1, -1),
        v_bias.reshape(1, -1),
        doc_ids.reshape(-1, HD),
        jnp.asarray(np.cos(inner), f32),
        jnp.asarray(np.sin(inner), f32),
        jnp.asarray(np.cos(outer), f32),
        jnp.asarray(np.sin(outer), f32),
    )


def solution(mesh):
    placed = (
        P("seq", None),
        P(),
        P(None, "tp"),
        P("tp"),
        P(None, "tp"),
        P("tp"),
        P(None, "tp"),
        P("tp"),
        P("tp", None),
        P(),
    )
    return jax.shard_map(
        body, mesh=mesh, in_specs=placed, out_specs=P("seq", "tp"), check_vma=False
    )
```
